32 devices in a mesh: groups: 2 (over x), freq: 8 (over z, y), gvec: 2 (over core).
Axes of the slice: x: 2, y: 2, z: 4, core: 2. Of those that a mesh axis runs over, the one named last changes fastest.
Arguments:
- screened: bfloat16 [16, 3072, 3072], P(('groups', 'freq'), 'gvec'), parts along dimension 0, may hold values from -0.109375 to 0.109375
- densities: bfloat16 [6144, 512], P(('groups', 'gvec'), 'freq'), parts along dimension 0, may hold values from -0.8046875 to 0.8046875
- pair_order: int32 [512], replicated, may hold values from 0 to 511, each once
- quad_index: int32 [4, 8], replicated, may hold values from 0 to 63
- quad_table: float32 [64], replicated, may hold values from 0.05 to 0.5
Outputs:
- kernel_out: float32 [8, 512, 512], P('groups', 'freq', 'gvec'), parts along dimension 0
The draws below stay inside these ranges and needn't reach their ends.
There are 2 independent parts, one for each index of `groups`. The reference program is written for one: setup_inputs(seed, part) draws one part's arguments, and reference() takes and returns one part's arrays. A program takes and returns all parts, laid end to end along the dimension named above; an argument that names none is the same for every part. Nothing has to cross between parts.
All inputs are finite; a program needn't handle non-finite values.
Results may differ from the reference program's by a relative error of at most 0.0029.
Values may be sent and summed in bfloat16 or wider, within the bound.
A program may use at most 64 MiB of HBM per device.

```python
import math
import jax
import jax.numpy as jnp
from jax import lax

GVECS = 3072
PAIRS = 512
ENERGIES = 4
QUAD_ROWS = 64
FREQS = 8


def place_ends(values, key, least, top_value):
    longest = values.shape.index(max(values.shape))
    spots = []
    for shift in (0, 1):
        where = [jax.random.randint(jax.random.fold_in(key, axis), (), 0, length) for axis, length in enumerate(values.shape)]
        where[longest] = (where[longest] + shift) % values.shape[longest]
        spots.append(tuple(where))
    return values.at[spots[0]].set(least).at[spots[1]].set(top_value)


def block_scale(stream_key, extent, shards, low, largest):
    loudness, own = 1.0, jax.random.fold_in(stream_key, 6)
    for dim, blocks in shards:
        steps = jnp.exp(jax.random.uniform(jax.random.fold_in(own, dim), (blocks,), jnp.float32, low / len(shards), largest / len(shards)))
        loudness = loudness * jnp.repeat(steps, extent[dim] // blocks).reshape([-1 if axis == dim else 1 for axis in range(len(extent))])
    return loudness


def normal_values(own_key, extent, spread, reach, cuts=(), kind=jnp.bfloat16):
    entries = spread * jax.random.normal(own_key, extent, jnp.float32)
    if cuts:
        entries = entries * block_scale(own_key, extent, cuts, -0.22, 0.18)
    return jnp.clip(entries, -reach, reach).astype(kind)


def setup_inputs(seed: int = 0, part: int = 0) -> dict:
    key_list = jax.random.split(jax.random.key(seed), 6)
    part_splits = jax.random.split(jax.random.fold_in(key_list[5], part), 6)
    screened = normal_values(part_splits[0], (FREQS, GVECS, GVECS), GVECS ** -0.5, 0.109375, ((0, 8), (1, 2)))
    densities = normal_values(part_splits[1], (GVECS, PAIRS), (GVECS ** -0.25), 0.8046875, ((0, 2), (1, 8)))
    pair_order = jax.random.permutation(key_list[2], PAIRS).astype(jnp.int32)
    quad_index = place_ends(jax.random.randint(key_list[3], (ENERGIES, FREQS), 0, QUAD_ROWS), jax.random.fold_in(key_list[3], 1), 0, QUAD_ROWS - 1).astype(jnp.int32)
    quad_table = jnp.clip(jnp.exp(jax.random.uniform(key_list[4], (QUAD_ROWS,), jnp.float32, math.log(0.05), math.log(0.5))), 0.05, 0.5)
    return {"screened": screened, "densities": densities, "pair_order": pair_order, "quad_index": quad_index, "quad_table": quad_table}


def reference(screened, densities, pair_order, quad_index, quad_table):
    ordered = jnp.take(densities, pair_order, axis=1)
    weights = quad_table[quad_index]

    def advance(running, inputs):
        screen_now, weight_now = inputs
        product = jnp.dot(screen_now, ordered, preferred_element_type=jnp.float32).astype(jnp.bfloat16)
        kernel = jnp.dot(ordered.T, product, preferred_element_type=jnp.float32)
        return running + weight_now[:, None, None] * kernel, None

    start_value = jnp.zeros((ENERGIES, PAIRS, PAIRS), jnp.float32)
    running, unused = lax.scan(advance, start_value, (screened, weights.T))
    return running
```

```python
import functools

import jax
import jax.numpy as jnp
from jax import lax
from jax.experimental import pallas as pl
from jax.experimental.pallas import tpu as pltpu
from jax.sharding import PartitionSpec as P

MESH = pl.DeviceIdType.MESH
F32 = jnp.float32
BF16 = jnp.bfloat16
NT = (((1,), (1,)), ((), ()))


def kernel(
    n, chunks, screened, dens, order, quad_index, quad_table, out,
    w_buf, x_buf, e_buf, acc, pa_buf, p_buf, perm, order_rows, k_send, k_peer, k_own, k_red, rows_in,
    own_sem, w_sem, ring_send, ring_recv, own_send, own_recv, pair_send, pair_recv,
    half_send, half_recv, out_send, out_recv,
):
    per, rows = dens.shape
    pairs = n * per
    half = pairs // 2
    mid = n // 2
    width = rows // chunks
    me = lax.axis_index("freq")
    core = lax.axis_index("gvec")
    peer = 1 - core

    def index_at(position):
        fold = position // mid
        return (1 - fold) * (2 * position) + fold * (2 * (n - 1 - position) + 1)

    odd = me % 2
    place = (1 - odd) * (me // 2) + odd * (n - 1 - me // 2)
    right = index_at((place + 1) % n)
    left = index_at((place + n - 1) % n)

    own_copy = pltpu.make_async_copy(dens, x_buf.at[core, 0:per, :], own_sem.at[0])
    own_copy.start()

    barrier = pltpu.get_barrier_semaphore()
    pl.semaphore_signal(barrier, inc=1, device_id={"freq": left}, device_id_type=MESH)
    pl.semaphore_signal(barrier, inc=1, device_id={"freq": right}, device_id_type=MESH)
    pl.semaphore_signal(barrier, inc=1, device_id={"gvec": peer}, device_id_type=MESH)

    def w_copy(h):
        return pltpu.make_async_copy(
            screened.at[0, :, pl.ds(h * rows, rows)], w_buf.at[h], w_sem.at[h]
        )

    mine = pl.ds(pl.multiple_of(me * per, per), per)

    def lanes(c, count=1):
        return pl.ds(c * width, count * width)

    def spot(d, side):
        return n - 1 if d == mid else max(0, 2 * d - 1 + side)

    def block(c, at, half_of):
        return x_buf.at[half_of, pl.ds(at * per, per), lanes(c)]

    def ring_copy(c, d, side):
        return pltpu.make_async_remote_copy(
            src_ref=block(c, spot(d, side), core), dst_ref=block(c, spot(d + 1, side), core),
            send_sem=ring_send.at[c, side * mid + d], recv_sem=ring_recv.at[c, side * mid + d],
            device_id={"freq": left if side else right}, device_id_type=MESH,
        )

    def pair_copy(c, at, half_of):
        ref = block(c, at, half_of)
        return pltpu.make_async_remote_copy(
            src_ref=ref, dst_ref=ref, send_sem=pair_send.at[c, at],
            recv_sem=pair_recv.at[c, at], device_id={"gvec": peer}, device_id_type=MESH,
        )

    def own_pair(half_of):
        ref = x_buf.at[half_of, 0:per, :]
        return pltpu.make_async_remote_copy(
            src_ref=ref, dst_ref=ref, send_sem=own_send.at[0],
            recv_sem=own_recv.at[0], device_id={"gvec": peer}, device_id_type=MESH,
        )

    evens, odds = list(range(0, chunks, 2)), list(range(1, chunks, 2))
    sequence = (evens + odds, odds + evens)

    def reach(c, side):
        return mid if c % 2 == side else mid - 1

    own_copy.wait()
    pl.semaphore_wait(barrier, 3)
    for i in range(chunks):
        for side in range(2):
            ring_copy(sequence[side][i], 0, side).start()
    own_pair(core).start()
    for h in range(2):
        w_copy(h).start()

    for at in range(n):
        d, side = (at + 1) // 2, 1 - at % 2
        origin = index_at((place + (d if side else n - d)) % n)
        pair = lax.broadcasted_iota(jnp.int32, (per, pairs), 0) + origin * per
        one_hot = (pair == order[...]).astype(F32)
        order_rows[at * per:(at + 1) * per, :] = one_hot.astype(BF16)
    perm[...] = order_rows[...].astype(F32).T.astype(BF16)

    groups = (slice(0, half), slice(half, pairs))
    joined = 2 if chunks % 2 == 0 else 1
    spans = [lanes(c, joined) for c in range(0, chunks, joined)]
    seen = set()

    def have(g, j):
        for at in range(g * mid, (g + 1) * mid):
            for c in range(j * joined, (j + 1) * joined):
                key = (0, 0) if at == 0 else (c, at)
                if key not in seen:
                    seen.add(key)
                    if at == 0:
                        own_pair(peer).wait_recv()
                    else:
                        pair_copy(c, at, peer).wait_recv()

    def have_w():
        if "w" not in seen:
            seen.add("w")
            for h in range(2):
                w_copy(h).wait()

    tile = rows // 2 if rows % 32 == 0 else rows
    tiles = [slice(r, r + tile) for r in range(0, rows, tile)]

    def term(g, j, h, at):
        return lax.dot_general(
            w_buf[h, at, spans[j]], x_buf[h, groups[g], spans[j]], NT, preferred_element_type=F32
        )

    def turned(g, at, total):
        total = total.astype(BF16)
        for h in range(2):
            part = jnp.dot(
                total, order_rows[groups[g], h * half:(h + 1) * half], preferred_element_type=F32
            )
            if g == 0:
                pa_buf[h, at, :] = part.astype(BF16)
            else:
                p_buf[h, at, :] = (part + pa_buf[h, at, :].astype(F32)).astype(BF16)

    def early(j, at):
        def run():
            have_w()
            have(0, j)
            total = term(0, j, 0, at) + term(0, j, 1, at)
            if j > 0:
                total = total + acc[0, at, :]
            if j < len(spans) - 1:
                acc[0, at, :] = total
            else:
                turned(0, at, total)
        return run

    def late_own(j):
        def run():
            have_w()
            for at in tiles:
                total = term(1, j, core, at)
                if j > 0:
                    total = total + acc[1, at, :]
                acc[1, at, :] = total
        return run

    def late_peer(j):
        def run():
            have(1, j)
            for at in tiles:
                total = acc[1, at, :] + term(1, j, peer, at)
                if j < len(spans) - 1:
                    acc[1, at, :] = total
                else:
                    turned(1, at, total)
        return run

    def order_own(g, j):
        def run():
            part = jnp.dot(
                perm[:, groups[g]], x_buf[core, groups[g], spans[j]], preferred_element_type=F32
            )
            if g == 1:
                part = part + e_buf[:, spans[j]].astype(F32)
            e_buf[:, spans[j]] = part.astype(BF16)
        return run

    def arrival(j, d, side):
        return max(
            (d - 1) * chunks + sequence[side].index(c)
            for c in range(j * joined, (j + 1) * joined) if c % 2 == side or d < mid
        )

    todo = []
    turn = mid // 2
    for j in range(len(spans)):
        for at in tiles:
            todo.append((arrival(j, turn, 0) + 1, early(j, at)))
    for j in range(len(spans)):
        todo.append((arrival(j, turn, 0), order_own(0, j)))
    for j in range(len(spans)):
        last = max(
            (mid - 1) * chunks + sequence[c % 2].index(c) for c in range(j * joined, (j + 1) * joined)
        )
        todo.append((last, late_own(j)))
        todo.append((last, order_own(1, j)))
        todo.append((last + 1, late_peer(j)))

    slot = 0
    for d in range(1, mid + 1):
        for i in range(chunks):
            moved = False
            for side in range(2):
                c = sequence[side][i]
                if d <= reach(c, side):
                    moved = True
                    ring_copy(c, d - 1, side).wait_recv()
                    if d < reach(c, side):
                        ring_copy(c, d, side).start()
                    pair_copy(c, spot(d, side), core).start()
            if moved and todo and todo[0][0] <= slot:
                todo.pop(0)[1]()
            slot += 1
    for _, run in todo:
        run()

    size = k_send.shape[1]
    count = size // per
    near = me // mid
    local = me % mid
    pieces = []
    for b in (1 - near, near):
        for s in range(half // size):
            pieces.append((b, s))

    def piece_rows(b, s):
        return pl.ds(pl.multiple_of(b * half + s * size, size), size)

    def half_copy(i):
        return pltpu.make_async_remote_copy(
            src_ref=k_send.at[i], dst_ref=k_peer.at[i], send_sem=half_send.at[i],
            recv_sem=half_recv.at[i], device_id={"gvec": peer}, device_id_type=MESH,
        )

    def out_copy(target, slot):
        return pltpu.make_async_remote_copy(
            src_ref=k_red.at[pl.ds(pl.multiple_of(target * per, per), per), :],
            dst_ref=rows_in.at[me], send_sem=out_send.at[slot], recv_sem=out_recv.at[me],
            device_id={"freq": target}, device_id_type=MESH,
        )

    for i, (b, s) in enumerate(pieces):
        k_send[i] = jnp.dot(e_buf[piece_rows(b, s), :], p_buf[peer], preferred_element_type=F32)
        half_copy(i).start()
    for i, (b, s) in enumerate(pieces):
        k_own[i] = jnp.dot(e_buf[piece_rows(b, s), :], p_buf[core], preferred_element_type=F32)
    sent = 0
    targets = []
    for i, (b, s) in enumerate(pieces):
        half_copy(i).wait_recv()
        k_red[piece_rows(b, s), :] = (k_own[i] + k_peer[i]).astype(BF16)
        for t in range(count):
            target = b * mid + s * count + (local + t) % count
            if i < half // size:
                out_copy(target, sent).start()
            else:
                @pl.when(target != me)
                def _():
                    out_copy(target, sent).start()
            targets.append(target)
            sent += 1
    rows_in[me] = k_red[mine, :]

    def arrived(t):
        source = near * mid + (local + t) % mid if t < mid else (1 - near) * mid + (local + t) % mid
        pltpu.make_async_remote_copy(
            src_ref=rows_in.at[source], dst_ref=rows_in.at[source],
            send_sem=out_send.at[0], recv_sem=out_recv.at[source],
            device_id={"freq": source}, device_id_type=MESH,
        ).wait_recv()
        return source

    def weighted(o, sources):
        return sum(quad_table[quad_index[o, f]] * rows_in[f].astype(F32) for f in sources)

    sources = [me]
    for t in range(1, mid):
        sources.append(arrived(t))
    for o in range(out.shape[0]):
        out[o] = weighted(o, sources)
    sources = [arrived(t) for t in range(mid, n)]
    for o in range(out.shape[0]):
        out[o] = out[o] + weighted(o, sources)

    for c in range(chunks):
        for side in range(2):
            for d in range(reach(c, side)):
                ring_copy(c, d, side).wait_send()
        for at in range(1, n):
            pair_copy(c, at, core).wait_send()
    own_pair(core).wait_send()
    for i in range(len(pieces)):
        half_copy(i).wait_send()
    for slot, target in enumerate(targets):
        if slot < mid:
            out_copy(target, slot).wait_send()
        else:
            @pl.when(target != me)
            def _():
                out_copy(target, slot).wait_send()


def body(n, screened, densities, pair_order, quad_index, quad_table):
    rows, per = densities.shape
    pairs = n * per
    half = pairs // 2
    mid = n // 2
    chunks = next(c for c in (4, 3, 2, 1) if rows % (c * 128) == 0 or c == 1)
    width = rows // chunks
    size = half // 2 if mid % 2 == 0 and (half // 2) % 16 == 0 else half
    count = half // size * 2
    energies = quad_index.shape[0]
    dma = pltpu.SemaphoreType.DMA
    hbm = pl.BlockSpec(memory_space=pl.ANY)
    vmem = pl.BlockSpec(memory_space=pltpu.VMEM)
    smem = pl.BlockSpec(memory_space=pltpu.SMEM)
    return pl.pallas_call(
        functools.partial(kernel, n, chunks),
        out_shape=pltpu.VMEM((energies, per, half), F32),
        in_specs=[hbm, hbm, vmem, smem, smem],
        out_specs=vmem,
        scratch_shapes=[
            pltpu.VMEM((2, rows, rows), BF16),
            pltpu.VMEM((2, pairs, rows), BF16),
            pltpu.VMEM((pairs, rows), BF16),
            pltpu.VMEM((2, rows, half), F32),
            pltpu.VMEM((2, rows, half), BF16),
            pltpu.VMEM((2, rows, half), BF16),
            pltpu.VMEM((pairs, pairs), BF16),
            pltpu.VMEM((pairs, pairs), BF16),
            pltpu.VMEM((count, size, half), F32),
            pltpu.VMEM((count, size, half), F32),
            pltpu.VMEM((count, size, half), F32),
            pltpu.VMEM((pairs, half), BF16),
            pltpu.VMEM((n, per, half), BF16),
            dma((1,)), dma((2,)),
            dma((chunks, n)), dma((chunks, n)),
            dma((1,)), dma((1,)),
            dma((chunks, n)), dma((chunks, n)),
            dma((count,)), dma((count,)), dma((n,)), dma((n,)),
        ],
        compiler_params=pltpu.CompilerParams(
            collective_id=0, has_side_effects=True, vmem_limit_bytes=56 * 1024 * 1024
        ),
    )(screened, densities.T, pair_order[None, :], quad_index, quad_table)


def solution(mesh):
    placed = (P(("groups", "freq"), "gvec", None), P(("groups", "gvec"), "freq"), P(), P(), P())
    return jax.shard_map(
        functools.partial(body, mesh.shape["freq"]), mesh=mesh, in_specs=placed,
        out_specs=P("groups", "freq", "gvec"), check_vma=False,
    )
```

```python
import functools

import jax
import jax.numpy as jnp
from jax import lax
from jax.experimental import pallas as pl
from jax.experimental.pallas import tpu as pltpu
from jax.sharding import PartitionSpec as P

MESH = pl.DeviceIdType.MESH
F32 = jnp.float32
BF16 = jnp.bfloat16
NT = (((1,), (1,)), ((), ()))


def kernel(
    n, chunks, screened, dens, order, quad_index, quad_table, out,
    w_buf, x_buf, e_buf, acc, pa_buf, p_buf, perm, order_rows, k_send, k_peer, k_own, k_red, rows_in,
    own_sem, w_sem, ring_send, ring_recv, own_send, own_recv, pair_send, pair_recv,
    half_send, half_recv, out_send, out_recv,
):
    per, rows = dens.shape
    pairs = n * per
    half = pairs // 2
    mid = n // 2
    width = rows // chunks
    me = lax.axis_index("freq")
    core = lax.axis_index("gvec")
    peer = 1 - core

    def index_at(position):
        fold = position // mid
        return (1 - fold) * (2 * position) + fold * (2 * (n - 1 - position) + 1)

    odd = me % 2
    place = (1 - odd) * (me // 2) + odd * (n - 1 - me // 2)
    right = index_at((place + 1) % n)
    left = index_at((place + n - 1) % n)

    own_copy = pltpu.make_async_copy(dens, x_buf.at[core, 0:per, :], own_sem.at[0])
    own_copy.start()

    barrier = pltpu.get_barrier_semaphore()
    pl.semaphore_signal(barrier, inc=1, device_id={"freq": left}, device_id_type=MESH)
    pl.semaphore_signal(barrier, inc=1, device_id={"freq": right}, device_id_type=MESH)
    pl.semaphore_signal(barrier, inc=1, device_id={"gvec": peer}, device_id_type=MESH)

    def w_copy(h):
        return pltpu.make_async_copy(
            screened.at[0, :, pl.ds(h * rows, rows)], w_buf.at[h], w_sem.at[h]
        )

    mine = pl.ds(pl.multiple_of(me * per, per), per)

    def lanes(c, count=1):
        return pl.ds(c * width, count * width)

    def spot(d, side):
        return n - 1 if d == mid else max(0, 2 * d - 1 + side)

    def block(c, at, half_of):
        return x_buf.at[half_of, pl.ds(at * per, per), lanes(c)]

    def ring_copy(c, d, side):
        return pltpu.make_async_remote_copy(
            src_ref=block(c, spot(d, side), core), dst_ref=block(c, spot(d + 1, side), core),
            send_sem=ring_send.at[c, side * mid + d], recv_sem=ring_recv.at[c, side * mid + d],
            device_id={"freq": left if side else right}, device_id_type=MESH,
        )

    def pair_copy(c, at, half_of):
        ref = block(c, at, half_of)
        return pltpu.make_async_remote_copy(
            src_ref=ref, dst_ref=ref, send_sem=pair_send.at[c, at],
            recv_sem=pair_recv.at[c, at], device_id={"gvec": peer}, device_id_type=MESH,
        )

    def own_pair(half_of):
        ref = x_buf.at[half_of, 0:per, :]
        return pltpu.make_async_remote_copy(
            src_ref=ref, dst_ref=ref, send_sem=own_send.at[0],
            recv_sem=own_recv.at[0], device_id={"gvec": peer}, device_id_type=MESH,
        )

    evens, odds = list(range(0, chunks, 2)), list(range(1, chunks, 2))
    sequence = (evens + odds, odds + evens)

    def reach(c, side):
        return mid if c % 2 == side else mid - 1

    own_copy.wait()
    pl.semaphore_wait(barrier, 3)
    for i in range(chunks):
        for side in range(2):
            ring_copy(sequence[side][i], 0, side).start()
    own_pair(core).start()
    for h in range(2):
        w_copy(h).start()

    for at in range(n):
        d, side = (at + 1) // 2, 1 - at % 2
        origin = index_at((place + (d if side else n - d)) % n)
        pair = lax.broadcasted_iota(jnp.int32, (per, pairs), 0) + origin * per
        one_hot = (pair == order[...]).astype(F32)
        order_rows[at * per:(at + 1) * per, :] = one_hot.astype(BF16)
    perm[...] = order_rows[...].astype(F32).T.astype(BF16)

    groups = (slice(0, half), slice(half, pairs))
    joined = 2 if chunks % 2 == 0 else 1
    spans = [lanes(c, joined) for c in range(0, chunks, joined)]
    seen = set()

    def have(g, j):
        for at in range(g * mid, (g + 1) * mid):
            for c in range(j * joined, (j + 1) * joined):
                key = (0, 0) if at == 0 else (c, at)
                if key not in seen:
                    seen.add(key)
                    if at == 0:
                        own_pair(peer).wait_recv()
                    else:
                        pair_copy(c, at, peer).wait_recv()

    def have_w():
        if "w" not in seen:
            seen.add("w")
            for h in range(2):
                w_copy(h).wait()

    tile = rows // 2 if rows % 32 == 0 else rows
    tiles = [slice(r, r + tile) for r in range(0, rows, tile)]

    def term(g, j, h, at):
        return lax.dot_general(
            w_buf[h, at, spans[j]], x_buf[h, groups[g], spans[j]], NT, preferred_element_type=F32
        )

    def turned(g, at, total):
        total = total.astype(BF16)
        for h in range(2):
            part = jnp.dot(
                total, order_rows[groups[g], h * half:(h + 1) * half], preferred_element_type=F32
            )
            if g == 0:
                pa_buf[h, at, :] = part.astype(BF16)
            else:
                p_buf[h, at, :] = (part + pa_buf[h, at, :].astype(F32)).astype(BF16)

    def early(j):
        def run():
            have_w()
            have(0, j)
            for at in tiles:
                total = term(0, j, 0, at) + term(0, j, 1, at)
                if j > 0:
                    total = total + acc[0, at, :]
                if j < len(spans) - 1:
                    acc[0, at, :] = total
                else:
                    turned(0, at, total)
        return run

    def late(j):
        def run():
            have_w()
            if j > 0:
                have(1, j - 1)
            for at in tiles:
                parts = []
                if j > 0:
                    parts = [acc[1, at, :], term(1, j - 1, peer, at)]
                if j < len(spans):
                    acc[1, at, :] = sum(parts + [term(1, j, core, at)])
                else:
                    turned(1, at, sum(parts))
        return run

    def order_own(g, j):
        def run():
            part = jnp.dot(
                perm[:, groups[g]], x_buf[core, groups[g], spans[j]], preferred_element_type=F32
            )
            if g == 1:
                part = part + e_buf[:, spans[j]].astype(F32)
            e_buf[:, spans[j]] = part.astype(BF16)
        return run

    def arrival(j, d):
        return max(
            (d - 1) * chunks + sequence[side].index(c)
            for c in range(j * joined, (j + 1) * joined) for side in range(2)
            if d < mid or c % 2 == side
        )

    turn = (mid + 1) // 2
    todo = []
    for j in range(len(spans)):
        todo.append((arrival(j, turn) + 1 + j, early(j)))
        todo.append((arrival(j, turn) + 2 + j, order_own(0, j)))
    for j in range(len(spans)):
        todo.append((arrival(j, mid), late(j)))
        todo.append((arrival(j, mid), order_own(1, j)))
    todo.append((mid * chunks, late(len(spans))))

    slot = 0
    for d in range(1, mid + 1):
        for i in range(chunks):
            moved = False
            for side in range(2):
                c = sequence[side][i]
                if d <= reach(c, side):
                    moved = True
                    ring_copy(c, d - 1, side).wait_recv()
                    if d < reach(c, side):
                        ring_copy(c, d, side).start()
                    pair_copy(c, spot(d, side), core).start()
            if moved and todo and todo[0][0] <= slot:
                todo.pop(0)[1]()
            slot += 1
    for _, run in todo:
        run()

    size = k_send.shape[1]
    count = size // per
    near = me // mid
    local = me % mid
    parts = half // size
    pieces = []
    for b in (1 - near, near):
        for s in range(parts):
            pieces.append((b, s + b * (parts - 1 - 2 * s)))

    def piece_rows(b, s):
        return pl.ds(pl.multiple_of(b * half + s * size, size), size)

    def half_copy(i):
        return pltpu.make_async_remote_copy(
            src_ref=k_send.at[i], dst_ref=k_peer.at[i], send_sem=half_send.at[i],
            recv_sem=half_recv.at[i], device_id={"gvec": peer}, device_id_type=MESH,
        )

    def out_copy(target, slot):
        return pltpu.make_async_remote_copy(
            src_ref=k_red.at[pl.ds(pl.multiple_of(target * per, per), per), :],
            dst_ref=rows_in.at[me], send_sem=out_send.at[slot], recv_sem=out_recv.at[me],
            device_id={"freq": target}, device_id_type=MESH,
        )

    far = half // size
    for stage in (range(far), range(far, len(pieces))):
        for i in stage:
            k_send[i] = jnp.dot(e_buf[piece_rows(*pieces[i]), :], p_buf[peer], preferred_element_type=F32)
            half_copy(i).start()
        for i in stage:
            k_own[i] = jnp.dot(e_buf[piece_rows(*pieces[i]), :], p_buf[core], preferred_element_type=F32)
    sent = 0
    targets = []
    for i, (b, s) in enumerate(pieces):
        half_copy(i).wait_recv()
        k_red[piece_rows(b, s), :] = (k_own[i] + k_peer[i]).astype(BF16)
        if i % parts == parts - 1:
            for t in range(mid):
                first, second = t // parts, t % parts
                place_s = pieces[i - parts + 1 + second][1]
                target = b * mid + place_s * count + first
                if i < parts:
                    out_copy(target, sent).start()
                else:
                    @pl.when(target != me)
                    def _():
                        out_copy(target, sent).start()
                targets.append(target)
                sent += 1
    rows_in[me] = k_red[mine, :]

    def arrived(t):
        source = near * mid + (local + t) % mid if t < mid else (1 - near) * mid + (local + t) % mid
        pltpu.make_async_remote_copy(
            src_ref=rows_in.at[source], dst_ref=rows_in.at[source],
            send_sem=out_send.at[0], recv_sem=out_recv.at[source],
            device_id={"freq": source}, device_id_type=MESH,
        ).wait_recv()
        return source

    def weighted(o, sources):
        return sum(quad_table[quad_index[o, f]] * rows_in[f].astype(F32) for f in sources)

    sources = [me]
    for t in range(1, mid):
        sources.append(arrived(t))
    for o in range(out.shape[0]):
        out[o] = weighted(o, sources)
    sources = [arrived(t) for t in range(mid, n)]
    for o in range(out.shape[0]):
        out[o] = out[o] + weighted(o, sources)

    for c in range(chunks):
        for side in range(2):
            for d in range(reach(c, side)):
                ring_copy(c, d, side).wait_send()
        for at in range(1, n):
            pair_copy(c, at, core).wait_send()
    own_pair(core).wait_send()
    for i in range(len(pieces)):
        half_copy(i).wait_send()
    for slot, target in enumerate(targets):
        if slot < mid:
            out_copy(target, slot).wait_send()
        else:
            @pl.when(target != me)
            def _():
                out_copy(target, slot).wait_send()


def body(n, screened, densities, pair_order, quad_index, quad_table):
    rows, per = densities.shape
    pairs = n * per
    half = pairs // 2
    mid = n // 2
    chunks = next(c for c in (4, 3, 2, 1) if rows % (c * 128) == 0 or c == 1)
    width = rows // chunks
    size = half // 2 if mid % 2 == 0 and (half // 2) % 16 == 0 else half
    count = half // size * 2
    energies = quad_index.shape[0]
    dma = pltpu.SemaphoreType.DMA
    hbm = pl.BlockSpec(memory_space=pl.ANY)
    vmem = pl.BlockSpec(memory_space=pltpu.VMEM)
    smem = pl.BlockSpec(memory_space=pltpu.SMEM)
    return pl.pallas_call(
        functools.partial(kernel, n, chunks),
        out_shape=pltpu.VMEM((energies, per, half), F32),
        in_specs=[hbm, hbm, vmem, smem, smem],
        out_specs=vmem,
        scratch_shapes=[
            pltpu.VMEM((2, rows, rows), BF16),
            pltpu.VMEM((2, pairs, rows), BF16),
            pltpu.VMEM((pairs, rows), BF16),
            pltpu.VMEM((2, rows, half), F32),
            pltpu.VMEM((2, rows, half), BF16),
            pltpu.VMEM((2, rows, half), BF16),
            pltpu.VMEM((pairs, pairs), BF16),
            pltpu.VMEM((pairs, pairs), BF16),
            pltpu.VMEM((count, size, half), F32),
            pltpu.VMEM((count, size, half), F32),
            pltpu.VMEM((count, size, half), F32),
            pltpu.VMEM((pairs, half), BF16),
            pltpu.VMEM((n, per, half), BF16),
            dma((1,)), dma((2,)),
            dma((chunks, n)), dma((chunks, n)),
            dma((1,)), dma((1,)),
            dma((chunks, n)), dma((chunks, n)),
            dma((count,)), dma((count,)), dma((n,)), dma((n,)),
        ],
        compiler_params=pltpu.CompilerParams(
            collective_id=0, has_side_effects=True, vmem_limit_bytes=56 * 1024 * 1024
        ),
    )(screened, densities.T, pair_order[None, :], quad_index, quad_table)


def solution(mesh):
    placed = (P(("groups", "freq"), "gvec", None), P(("groups", "gvec"), "freq"), P(), P(), P())
    return jax.shard_map(
        functools.partial(body, mesh.shape["freq"]), mesh=mesh, in_specs=placed,
        out_specs=P("groups", "freq", "gvec"), check_vma=False,
    )
```

```python
import functools

import jax
import jax.numpy as jnp
from jax import lax
from jax.experimental import pallas as pl
from jax.experimental.pallas import tpu as pltpu
from jax.sharding import PartitionSpec as P

MESH = pl.DeviceIdType.MESH
F32 = jnp.float32
BF16 = jnp.bfloat16
NT = (((1,), (1,)), ((), ()))


def kernel(
    n, chunks, screened, dens, order, quad_index, quad_table, out,
    w_buf, x_buf, e_buf, acc, pa_buf, p_buf, perm, order_rows, k_send, k_peer, k_own, k_red, rows_in,
    own_sem, w_sem, ring_send, ring_recv, own_send, own_recv, pair_send, pair_recv,
    half_send, half_recv, out_send, out_recv,
):
    per, rows = dens.shape
    pairs = n * per
    half = pairs // 2
    mid = n // 2
    width = rows // chunks
    me = lax.axis_index("freq")
    core = lax.axis_index("gvec")
    peer = 1 - core

    def index_at(position):
        fold = position // mid
        return (1 - fold) * (2 * position) + fold * (2 * (n - 1 - position) + 1)

    odd = me % 2
    place = (1 - odd) * (me // 2) + odd * (n - 1 - me // 2)
    right = index_at((place + 1) % n)
    left = index_at((place + n - 1) % n)

    own_copy = pltpu.make_async_copy(dens, x_buf.at[core, 0:per, :], own_sem.at[0])
    own_copy.start()

    barrier = pltpu.get_barrier_semaphore()
    pl.semaphore_signal(barrier, inc=1, device_id={"freq": left}, device_id_type=MESH)
    pl.semaphore_signal(barrier, inc=1, device_id={"freq": right}, device_id_type=MESH)
    pl.semaphore_signal(barrier, inc=1, device_id={"gvec": peer}, device_id_type=MESH)

    def w_copy(h):
        return pltpu.make_async_copy(
            screened.at[0, :, pl.ds(h * rows, rows)], w_buf.at[h], w_sem.at[h]
        )

    mine = pl.ds(pl.multiple_of(me * per, per), per)

    def lanes(c, count=1):
        return pl.ds(c * width, count * width)

    def spot(d, side):
        return n - 1 if d == mid else max(0, 2 * d - 1 + side)

    def block(c, at, half_of):
        return x_buf.at[half_of, pl.ds(at * per, per), lanes(c)]

    def ring_copy(c, d, side):
        return pltpu.make_async_remote_copy(
            src_ref=block(c, spot(d, side), core), dst_ref=block(c, spot(d + 1, side), core),
            send_sem=ring_send.at[c, side * mid + d], recv_sem=ring_recv.at[c, side * mid + d],
            device_id={"freq": left if side else right}, device_id_type=MESH,
        )

    def pair_copy(c, at, half_of):
        ref = block(c, at, half_of)
        return pltpu.make_async_remote_copy(
            src_ref=ref, dst_ref=ref, send_sem=pair_send.at[c, at],
            recv_sem=pair_recv.at[c, at], device_id={"gvec": peer}, device_id_type=MESH,
        )

    def own_pair(half_of):
        ref = x_buf.at[half_of, 0:per, :]
        return pltpu.make_async_remote_copy(
            src_ref=ref, dst_ref=ref, send_sem=own_send.at[0],
            recv_sem=own_recv.at[0], device_id={"gvec": peer}, device_id_type=MESH,
        )

    evens, odds = list(range(0, chunks, 2)), list(range(1, chunks, 2))
    sequence = (evens + odds, odds + evens)

    def reach(c, side):
        return mid if c % 2 == side else mid - 1

    own_copy.wait()
    pl.semaphore_wait(barrier, 3)
    for i in range(chunks):
        for side in range(2):
            ring_copy(sequence[side][i], 0, side).start()
    own_pair(core).start()
    for h in range(2):
        w_copy(h).start()

    for at in range(n):
        d, side = (at + 1) // 2, 1 - at % 2
        origin = index_at((place + (d if side else n - d)) % n)
        pair = lax.broadcasted_iota(jnp.int32, (per, pairs), 0) + origin * per
        one_hot = (pair == order[...]).astype(F32)
        order_rows[at * per:(at + 1) * per, :] = one_hot.astype(BF16)
    perm[...] = order_rows[...].astype(F32).T.astype(BF16)

    groups = (slice(0, half), slice(half, pairs))
    joined = 2 if chunks % 2 == 0 else 1
    spans = [lanes(c, joined) for c in range(0, chunks, joined)]
    seen = set()

    def have(g, j):
        for at in range(g * mid, (g + 1) * mid):
            for c in range(j * joined, (j + 1) * joined):
                key = (0, 0) if at == 0 else (c, at)
                if key not in seen:
                    seen.add(key)
                    if at == 0:
                        own_pair(peer).wait_recv()
                    else:
                        pair_copy(c, at, peer).wait_recv()

    def have_w():
        if "w" not in seen:
            seen.add("w")
            for h in range(2):
                w_copy(h).wait()

    tile = rows // 2 if rows % 32 == 0 else rows
    tiles = [slice(r, r + tile) for r in range(0, rows, tile)]

    def term(g, j, h, at):
        return lax.dot_general(
            w_buf[h, at, spans[j]], x_buf[h, groups[g], spans[j]], NT, preferred_element_type=F32
        )

    def turned(g, at, total):
        total = total.astype(BF16)
        both = jnp.dot(total, order_rows[groups[g], :], preferred_element_type=F32).astype(BF16)
        for h in range(2):
            part = both[:, h * half:(h + 1) * half]
            if g == 0:
                pa_buf[h, at, :] = part
            else:
                p_buf[h, at, :] = part + pa_buf[h, at, :]

    def early(j):
        def run():
            have_w()
            have(0, j)
            for at in tiles:
                total = term(0, j, 0, at) + term(0, j, 1, at)
                if j > 0:
                    total = total + acc[0, at, :]
                if j < len(spans) - 1:
                    acc[0, at, :] = total
                else:
                    turned(0, at, total)
        return run

    def late(j):
        def run():
            have_w()
            if j > 0:
                have(1, j - 1)
            for at in tiles:
                parts = []
                if j > 0:
                    parts = [acc[1, at, :], term(1, j - 1, peer, at)]
                if j < len(spans):
                    acc[1, at, :] = sum(parts + [term(1, j, core, at)])
                else:
                    turned(1, at, sum(parts))
        return run

    def order_own(g, j):
        def run():
            part = jnp.dot(
                perm[:, groups[g]], x_buf[core, groups[g], spans[j]], preferred_element_type=F32
            )
            if g == 1:
                part = part + e_buf[:, spans[j]].astype(F32)
            e_buf[:, spans[j]] = part.astype(BF16)
        return run

    def arrival(j, d):
        return max(
            (d - 1) * chunks + sequence[side].index(c)
            for c in range(j * joined, (j + 1) * joined) for side in range(2)
            if d < mid or c % 2 == side
        )

    turn = (mid + 1) // 2
    todo = []
    for j in range(len(spans)):
        todo.append((arrival(j, turn) + 1 + j, early(j)))
        todo.append((arrival(j, turn) + 2 + j, order_own(0, j)))
    for j in range(len(spans)):
        todo.append((arrival(j, mid), late(j)))
        todo.append((arrival(j, mid), order_own(1, j)))
    todo.append((mid * chunks, late(len(spans))))

    slot = 0
    for d in range(1, mid + 1):
        for i in range(chunks):
            moved = False
            for side in range(2):
                c = sequence[side][i]
                if d <= reach(c, side):
                    moved = True
                    ring_copy(c, d - 1, side).wait_recv()
                    if d < reach(c, side):
                        ring_copy(c, d, side).start()
                    pair_copy(c, spot(d, side), core).start()
            if moved and todo and todo[0][0] <= slot:
                todo.pop(0)[1]()
                if d == mid and todo and todo[0][0] <= slot - i:
                    todo.pop(0)[1]()
            slot += 1
    for _, run in todo:
        run()

    size = k_send.shape[1]
    count = size // per
    near = me // mid
    local = me % mid
    parts = half // size
    pieces = []
    for b in range(2):
        for s in range(parts):
            pieces.append((b, s))

    def piece_rows(b, s):
        return pl.ds(pl.multiple_of(b * half + s * size, size), size)

    def half_copy(i):
        return pltpu.make_async_remote_copy(
            src_ref=k_send.at[i], dst_ref=k_peer.at[i], send_sem=half_send.at[i],
            recv_sem=half_recv.at[i], device_id={"gvec": peer}, device_id_type=MESH,
        )

    def out_copy(target, slot):
        return pltpu.make_async_remote_copy(
            src_ref=k_red.at[pl.ds(pl.multiple_of(target * per, per), per), :],
            dst_ref=rows_in.at[me], send_sem=out_send.at[slot], recv_sem=out_recv.at[me],
            device_id={"freq": target}, device_id_type=MESH,
        )

    far = half // size
    def emit(i):
        k_send[i] = jnp.dot(e_buf[piece_rows(*pieces[i]), :], p_buf[peer], preferred_element_type=F32)
        half_copy(i).start()

    def keep(i):
        k_own[i] = jnp.dot(e_buf[piece_rows(*pieces[i]), :], p_buf[core], preferred_element_type=F32)

    targets = []

    def finish(i):
        b, s = pieces[i]
        half_copy(i).wait_recv()
        k_red[piece_rows(b, s), :] = (k_own[i] + k_peer[i]).astype(BF16)
        for t in range(count):
            target = b * mid + s * count + t
            slot = len(targets)

            @pl.when(target != me)
            def _():
                out_copy(target, slot).start()

            targets.append(target)

    last = len(pieces)
    for i in range(last + 2):
        if i < last:
            emit(i)
            keep(i)
        if i >= 2:
            finish(i - 2)
    rows_in[me] = k_red[mine, :]

    def arrived(t):
        source = near * mid + (local + t) % mid if t < mid else (1 - near) * mid + (local + t) % mid
        pltpu.make_async_remote_copy(
            src_ref=rows_in.at[source], dst_ref=rows_in.at[source],
            send_sem=out_send.at[0], recv_sem=out_recv.at[source],
            device_id={"freq": source}, device_id_type=MESH,
        ).wait_recv()
        return source

    def weighted(o, sources):
        return sum(quad_table[quad_index[o, f]] * rows_in[f].astype(F32) for f in sources)

    sources = [me]
    for t in range(1, mid):
        sources.append(arrived(t))
    for o in range(out.shape[0]):
        out[o] = weighted(o, sources)
    sources = [arrived(t) for t in range(mid, n)]
    for o in range(out.shape[0]):
        out[o] = out[o] + weighted(o, sources)

    for c in range(chunks):
        for side in range(2):
            for d in range(reach(c, side)):
                ring_copy(c, d, side).wait_send()
        for at in range(1, n):
            pair_copy(c, at, core).wait_send()
    own_pair(core).wait_send()
    for i in range(len(pieces)):
        half_copy(i).wait_send()
    for slot, target in enumerate(targets):
        @pl.when(target != me)
        def _():
            out_copy(target, slot).wait_send()


def body(n, screened, densities, pair_order, quad_index, quad_table):
    rows, per = densities.shape
    pairs = n * per
    half = pairs // 2
    mid = n // 2
    chunks = next(c for c in (4, 3, 2, 1) if rows % (c * 128) == 0 or c == 1)
    width = rows // chunks
    size = half // 2 if mid % 2 == 0 and (half // 2) % 16 == 0 else half
    count = half // size * 2
    energies = quad_index.shape[0]
    dma = pltpu.SemaphoreType.DMA
    hbm = pl.BlockSpec(memory_space=pl.ANY)
    vmem = pl.BlockSpec(memory_space=pltpu.VMEM)
    smem = pl.BlockSpec(memory_space=pltpu.SMEM)
    return pl.pallas_call(
        functools.partial(kernel, n, chunks),
        out_shape=pltpu.VMEM((energies, per, half), F32),
        in_specs=[hbm, hbm, vmem, smem, smem],
        out_specs=vmem,
        scratch_shapes=[
            pltpu.VMEM((2, rows, rows), BF16),
            pltpu.VMEM((2, pairs, rows), BF16),
            pltpu.VMEM((pairs, rows), BF16),
            pltpu.VMEM((2, rows, half), F32),
            pltpu.VMEM((2, rows, half), BF16),
            pltpu.VMEM((2, rows, half), BF16),
            pltpu.VMEM((pairs, pairs), BF16),
            pltpu.VMEM((pairs, pairs), BF16),
            pltpu.VMEM((count, size, half), F32),
            pltpu.VMEM((count, size, half), F32),
            pltpu.VMEM((count, size, half), F32),
            pltpu.VMEM((pairs, half), BF16),
            pltpu.VMEM((n, per, half), BF16),
            dma((1,)), dma((2,)),
            dma((chunks, n)), dma((chunks, n)),
            dma((1,)), dma((1,)),
            dma((chunks, n)), dma((chunks, n)),
            dma((count,)), dma((count,)), dma((n,)), dma((n,)),
        ],
        compiler_params=pltpu.CompilerParams(
            collective_id=0, has_side_effects=True, vmem_limit_bytes=56 * 1024 * 1024
        ),
    )(screened, densities.T, pair_order[None, :], quad_index, quad_table)


def solution(mesh):
    placed = (P(("groups", "freq"), "gvec", None), P(("groups", "gvec"), "freq"), P(), P(), P())
    return jax.shard_map(
        functools.partial(body, mesh.shape["freq"]), mesh=mesh, in_specs=placed,
        out_specs=P("groups", "freq", "gvec"), check_vma=False,
    )
```

```python
import functools

import jax
import jax.numpy as jnp
from jax import lax
from jax.experimental import pallas as pl
from jax.experimental.pallas import tpu as pltpu
from jax.sharding import PartitionSpec as P

MESH = pl.DeviceIdType.MESH
F32 = jnp.float32
BF16 = jnp.bfloat16
NT = (((1,), (1,)), ((), ()))


def kernel(
    n, chunks, screened, dens, order, quad_index, quad_table, out,
    w_buf, x_buf, e_buf, acc, t_buf, pa_buf, p_buf, perm, order_rows, k_send, k_peer, k_own, k_red, rows_in,
    own_sem, w_sem, ring_send, ring_recv, own_send, own_recv, pair_send, pair_recv,
    half_send, half_recv, out_send, out_recv,
):
    per, rows = dens.shape
    pairs = n * per
    half = pairs // 2
    mid = n // 2
    width = rows // chunks
    me = lax.axis_index("freq")
    core = lax.axis_index("gvec")
    peer = 1 - core

    def index_at(position):
        fold = position // mid
        return (1 - fold) * (2 * position) + fold * (2 * (n - 1 - position) + 1)

    odd = me % 2
    place = (1 - odd) * (me // 2) + odd * (n - 1 - me // 2)
    right = index_at((place + 1) % n)
    left = index_at((place + n - 1) % n)

    own_copy = pltpu.make_async_copy(dens, x_buf.at[core, 0:per, :], own_sem.at[0])
    own_copy.start()

    barrier = pltpu.get_barrier_semaphore()
    pl.semaphore_signal(barrier, inc=1, device_id={"freq": left}, device_id_type=MESH)
    pl.semaphore_signal(barrier, inc=1, device_id={"freq": right}, device_id_type=MESH)
    pl.semaphore_signal(barrier, inc=1, device_id={"gvec": peer}, device_id_type=MESH)

    def w_copy(h):
        return pltpu.make_async_copy(
            screened.at[0, :, pl.ds(h * rows, rows)], w_buf.at[h], w_sem.at[h]
        )

    mine = pl.ds(pl.multiple_of(me * per, per), per)

    def lanes(c, count=1):
        return pl.ds(c * width, count * width)

    def spot(d, side):
        return n - 1 if d == mid else max(0, 2 * d - 1 + side)

    def block(c, at, half_of):
        return x_buf.at[half_of, pl.ds(at * per, per), lanes(c)]

    def ring_copy(c, d, side):
        return pltpu.make_async_remote_copy(
            src_ref=block(c, spot(d, side), core), dst_ref=block(c, spot(d + 1, side), core),
            send_sem=ring_send.at[c, side * mid + d], recv_sem=ring_recv.at[c, side * mid + d],
            device_id={"freq": left if side else right}, device_id_type=MESH,
        )

    def pair_copy(c, at, half_of):
        ref = block(c, at, half_of)
        return pltpu.make_async_remote_copy(
            src_ref=ref, dst_ref=ref, send_sem=pair_send.at[c, at],
            recv_sem=pair_recv.at[c, at], device_id={"gvec": peer}, device_id_type=MESH,
        )

    def own_pair(half_of):
        ref = x_buf.at[half_of, 0:per, :]
        return pltpu.make_async_remote_copy(
            src_ref=ref, dst_ref=ref, send_sem=own_send.at[0],
            recv_sem=own_recv.at[0], device_id={"gvec": peer}, device_id_type=MESH,
        )

    evens, odds = list(range(0, chunks, 2)), list(range(1, chunks, 2))
    sequence = (evens + odds, odds + evens)

    def reach(c, side):
        return mid if c % 2 == side else mid - 1

    own_copy.wait()
    pl.semaphore_wait(barrier, 3)
    for i in range(chunks):
        for side in range(2):
            ring_copy(sequence[side][i], 0, side).start()
    own_pair(core).start()
    for h in range(2):
        w_copy(h).start()

    for at in range(n):
        d, side = (at + 1) // 2, 1 - at % 2
        origin = index_at((place + (d if side else n - d)) % n)
        pair = lax.broadcasted_iota(jnp.int32, (per, pairs), 0) + origin * per
        one_hot = (pair == order[...]).astype(F32)
        order_rows[at * per:(at + 1) * per, :] = one_hot.astype(BF16)
    perm[...] = order_rows[...].astype(F32).T.astype(BF16)

    groups = (slice(0, half), slice(half, pairs))
    joined = 2 if chunks % 2 == 0 else 1
    spans = [lanes(c, joined) for c in range(0, chunks, joined)]
    seen = set()

    def have(g, j):
        for at in range(g * mid, (g + 1) * mid):
            for c in range(j * joined, (j + 1) * joined):
                key = (0, 0) if at == 0 else (c, at)
                if key not in seen:
                    seen.add(key)
                    if at == 0:
                        own_pair(peer).wait_recv()
                    else:
                        pair_copy(c, at, peer).wait_recv()

    def have_w():
        if "w" not in seen:
            seen.add("w")
            for h in range(2):
                w_copy(h).wait()

    tile = rows // 2 if rows % 32 == 0 else rows
    tiles = [slice(r, r + tile) for r in range(0, rows, tile)]

    def term(g, j, h, at):
        return lax.dot_general(
            w_buf[h, at, spans[j]], x_buf[h, groups[g], spans[j]], NT, preferred_element_type=F32
        )

    def turned(g):
        for at in tiles:
            both = jnp.dot(
                t_buf[g, at, :], order_rows[groups[g], :], preferred_element_type=F32
            ).astype(BF16)
            for h in range(2):
                part = both[:, h * half:(h + 1) * half]
                if g == 0:
                    pa_buf[h, at, :] = part
                else:
                    p_buf[h, at, :] = part + pa_buf[h, at, :]

    def early(j):
        def run():
            have_w()
            have(0, j)
            for at in tiles:
                total = term(0, j, 0, at) + term(0, j, 1, at)
                if j > 0:
                    total = total + acc[0, at, :]
                if j < len(spans) - 1:
                    acc[0, at, :] = total
                else:
                    t_buf[0, at, :] = total.astype(BF16)
            if j == len(spans) - 1:
                turned(0)
        return run

    def late(j):
        def run():
            have_w()
            if j > 0:
                have(1, j - 1)
            for at in tiles:
                parts = []
                if j > 0:
                    parts = [acc[1, at, :], term(1, j - 1, peer, at)]
                if j < len(spans):
                    acc[1, at, :] = sum(parts + [term(1, j, core, at)])
                else:
                    t_buf[1, at, :] = sum(parts).astype(BF16)
            if j == len(spans):
                turned(1)
        return run

    def order_own(g, j):
        def run():
            part = jnp.dot(
                perm[:, groups[g]], x_buf[core, groups[g], spans[j]], preferred_element_type=F32
            )
            if g == 1:
                part = part + e_buf[:, spans[j]].astype(F32)
            e_buf[:, spans[j]] = part.astype(BF16)
        return run

    def arrival(j, d):
        return max(
            (d - 1) * chunks + sequence[side].index(c)
            for c in range(j * joined, (j + 1) * joined) for side in range(2)
            if d < mid or c % 2 == side
        )

    turn = (mid + 1) // 2
    todo = []
    for j in range(len(spans)):
        todo.append((arrival(j, turn) + 1 + j, early(j)))
        todo.append((arrival(j, turn) + 2 + j, order_own(0, j)))
    for j in range(len(spans)):
        todo.append((arrival(j, mid), late(j)))
        todo.append((arrival(j, mid), order_own(1, j)))
    todo.append((mid * chunks, late(len(spans))))

    slot = 0
    for d in range(1, mid + 1):
        for i in range(chunks):
            moved = False
            for side in range(2):
                c = sequence[side][i]
                if d <= reach(c, side):
                    moved = True
                    ring_copy(c, d - 1, side).wait_recv()
                    if d < reach(c, side):
                        ring_copy(c, d, side).start()
                    pair_copy(c, spot(d, side), core).start()
            if moved and todo and todo[0][0] <= slot:
                todo.pop(0)[1]()
                if d == mid and todo and todo[0][0] <= slot - i:
                    todo.pop(0)[1]()
            slot += 1
    for _, run in todo:
        run()

    size = k_send.shape[1]
    count = size // per
    near = me // mid
    local = me % mid
    parts = half // size
    pieces = []
    for b in range(2):
        for s in range(parts):
            pieces.append((b, s))

    def piece_rows(b, s):
        return pl.ds(pl.multiple_of(b * half + s * size, size), size)

    def half_copy(i):
        return pltpu.make_async_remote_copy(
            src_ref=k_send.at[i], dst_ref=k_peer.at[i], send_sem=half_send.at[i],
            recv_sem=half_recv.at[i], device_id={"gvec": peer}, device_id_type=MESH,
        )

    def out_copy(target, slot):
        return pltpu.make_async_remote_copy(
            src_ref=k_red.at[pl.ds(pl.multiple_of(target * per, per), per), :],
            dst_ref=rows_in.at[me], send_sem=out_send.at[slot], recv_sem=out_recv.at[me],
            device_id={"freq": target}, device_id_type=MESH,
        )

    far = half // size
    def emit(i):
        k_send[i] = jnp.dot(e_buf[piece_rows(*pieces[i]), :], p_buf[peer], preferred_element_type=F32)
        half_copy(i).start()

    def keep(i):
        k_own[i] = jnp.dot(e_buf[piece_rows(*pieces[i]), :], p_buf[core], preferred_element_type=F32)

    targets = []

    def finish(i):
        b, s = pieces[i]
        half_copy(i).wait_recv()
        k_red[piece_rows(b, s), :] = (k_own[i] + k_peer[i]).astype(BF16)
        for t in range(count):
            target = b * mid + s * count + t
            slot = len(targets)

            @pl.when(target != me)
            def _():
                out_copy(target, slot).start()

            targets.append(target)

    last = len(pieces)
    for i in range(last + 2):
        if i < last:
            emit(i)
            keep(i)
        if i >= 2:
            finish(i - 2)
    rows_in[me] = k_red[mine, :]

    for c in range(chunks):
        for side in range(2):
            for d in range(reach(c, side)):
                ring_copy(c, d, side).wait_send()
        for at in range(1, n):
            pair_copy(c, at, core).wait_send()
    own_pair(core).wait_send()
    for i in range(len(pieces)):
        half_copy(i).wait_send()

    def arrived(t):
        source = near * mid + (local + t) % mid if t < mid else (1 - near) * mid + (local + t) % mid
        pltpu.make_async_remote_copy(
            src_ref=rows_in.at[source], dst_ref=rows_in.at[source],
            send_sem=out_send.at[0], recv_sem=out_recv.at[source],
            device_id={"freq": source}, device_id_type=MESH,
        ).wait_recv()
        return source

    def weighted(o, sources):
        return sum(quad_table[quad_index[o, f]] * rows_in[f].astype(F32) for f in sources)

    sources = [me]
    for t in range(1, mid):
        sources.append(arrived(t))
    for o in range(out.shape[0]):
        out[o] = weighted(o, sources)
    for t in range(mid, n, 2):
        sources = [arrived(t), arrived(t + 1)]
        for o in range(out.shape[0]):
            out[o] = out[o] + weighted(o, sources)

    for slot, target in enumerate(targets):
        @pl.when(target != me)
        def _():
            out_copy(target, slot).wait_send()


def body(n, screened, densities, pair_order, quad_index, quad_table):
    rows, per = densities.shape
    pairs = n * per
    half = pairs // 2
    mid = n // 2
    chunks = next(c for c in (4, 3, 2, 1) if rows % (c * 128) == 0 or c == 1)
    width = rows // chunks
    size = half // 2 if mid % 2 == 0 and (half // 2) % 16 == 0 else half
    count = half // size * 2
    energies = quad_index.shape[0]
    dma = pltpu.SemaphoreType.DMA
    hbm = pl.BlockSpec(memory_space=pl.ANY)
    vmem = pl.BlockSpec(memory_space=pltpu.VMEM)
    smem = pl.BlockSpec(memory_space=pltpu.SMEM)
    return pl.pallas_call(
        functools.partial(kernel, n, chunks),
        out_shape=pltpu.VMEM((energies, per, half), F32),
        in_specs=[hbm, hbm, vmem, smem, smem],
        out_specs=vmem,
        scratch_shapes=[
            pltpu.VMEM((2, rows, rows), BF16),
            pltpu.VMEM((2, pairs, rows), BF16),
            pltpu.VMEM((pairs, rows), BF16),
            pltpu.VMEM((2, rows, half), F32),
            pltpu.VMEM((2, rows, half), BF16),
            pltpu.VMEM((2, rows, half), BF16),
            pltpu.VMEM((2, rows, half), BF16),
            pltpu.VMEM((pairs, pairs), BF16),
            pltpu.VMEM((pairs, pairs), BF16),
            pltpu.VMEM((count, size, half), F32),
            pltpu.VMEM((count, size, half), F32),
            pltpu.VMEM((count, size, half), F32),
            pltpu.VMEM((pairs, half), BF16),
            pltpu.VMEM((n, per, half), BF16),
            dma((1,)), dma((2,)),
            dma((chunks, n)), dma((chunks, n)),
            dma((1,)), dma((1,)),
            dma((chunks, n)), dma((chunks, n)),
            dma((count,)), dma((count,)), dma((n,)), dma((n,)),
        ],
        compiler_params=pltpu.CompilerParams(
            collective_id=0, has_side_effects=True, vmem_limit_bytes=56 * 1024 * 1024
        ),
    )(screened, densities.T, pair_order[None, :], quad_index, quad_table)


def solution(mesh):
    placed = (P(("groups", "freq"), "gvec", None), P(("groups", "gvec"), "freq"), P(), P(), P())
    return jax.shard_map(
        functools.partial(body, mesh.shape["freq"]), mesh=mesh, in_specs=placed,
        out_specs=P("groups", "freq", "gvec"), check_vma=False,
    )
```

```python
import functools

import jax
import jax.numpy as jnp
from jax import lax
from jax.experimental import pallas as pl
from jax.experimental.pallas import tpu as pltpu
from jax.sharding import PartitionSpec as P

MESH = pl.DeviceIdType.MESH
F32 = jnp.float32
BF16 = jnp.bfloat16
NT = (((1,), (1,)), ((), ()))


def kernel(
    n, chunks, screened, dens, order, quad_index, quad_table, out,
    w_buf, x_buf, e_buf, acc, t_buf, pa_buf, p_buf, perm, order_rows, k_send, k_peer, k_own, k_red, rows_in,
    own_sem, w_sem, ring_send, ring_recv, own_send, own_recv, pair_send, pair_recv,
    half_send, half_recv, out_send, out_recv,
):
    per, rows = dens.shape
    pairs = n * per
    half = pairs // 2
    mid = n // 2
    width = rows // chunks
    me = lax.axis_index("freq")
    core = lax.axis_index("gvec")
    peer = 1 - core

    def index_at(position):
        fold = position // mid
        return (1 - fold) * (2 * position) + fold * (2 * (n - 1 - position) + 1)

    odd = me % 2
    place = (1 - odd) * (me // 2) + odd * (n - 1 - me // 2)
    right = index_at((place + 1) % n)
    left = index_at((place + n - 1) % n)

    own_copy = pltpu.make_async_copy(dens, x_buf.at[core, 0:per, :], own_sem.at[0])

    barrier = pltpu.get_barrier_semaphore()
    pl.semaphore_signal(barrier, inc=1, device_id={"freq": left}, device_id_type=MESH)
    pl.semaphore_signal(barrier, inc=1, device_id={"freq": right}, device_id_type=MESH)
    pl.semaphore_signal(barrier, inc=1, device_id={"gvec": peer}, device_id_type=MESH)
    own_copy.start()

    def w_copy(h):
        return pltpu.make_async_copy(
            screened.at[0, :, pl.ds(h * rows, rows)], w_buf.at[h], w_sem.at[h]
        )

    mine = pl.ds(pl.multiple_of(me * per, per), per)

    def lanes(c, count=1):
        return pl.ds(c * width, count * width)

    def spot(d, side):
        return n - 1 if d == mid else max(0, 2 * d - 1 + side)

    def block(c, at, half_of):
        return x_buf.at[half_of, pl.ds(at * per, per), lanes(c)]

    def ring_copy(c, d, side):
        return pltpu.make_async_remote_copy(
            src_ref=block(c, spot(d, side), core), dst_ref=block(c, spot(d + 1, side), core),
            send_sem=ring_send.at[c, side * mid + d], recv_sem=ring_recv.at[c, side * mid + d],
            device_id={"freq": left if side else right}, device_id_type=MESH,
        )

    def pair_copy(c, at, half_of):
        ref = block(c, at, half_of)
        return pltpu.make_async_remote_copy(
            src_ref=ref, dst_ref=ref, send_sem=pair_send.at[c, at],
            recv_sem=pair_recv.at[c, at], device_id={"gvec": peer}, device_id_type=MESH,
        )

    def own_pair(half_of):
        ref = x_buf.at[half_of, 0:per, :]
        return pltpu.make_async_remote_copy(
            src_ref=ref, dst_ref=ref, send_sem=own_send.at[0],
            recv_sem=own_recv.at[0], device_id={"gvec": peer}, device_id_type=MESH,
        )

    evens, odds = list(range(0, chunks, 2)), list(range(1, chunks, 2))
    sequence = (evens + odds, odds + evens)

    def reach(c, side):
        return mid if c % 2 == side else mid - 1

    own_copy.wait()
    pl.semaphore_wait(barrier, 3)
    for i in range(chunks):
        for side in range(2):
            ring_copy(sequence[side][i], 0, side).start()
    own_pair(core).start()
    for h in range(2):
        w_copy(h).start()

    for at in range(n):
        d, side = (at + 1) // 2, 1 - at % 2
        origin = index_at((place + (d if side else n - d)) % n)
        pair = lax.broadcasted_iota(jnp.int32, (per, pairs), 0) + origin * per
        one_hot = (pair == order[...]).astype(F32)
        order_rows[at * per:(at + 1) * per, :] = one_hot.astype(BF16)
    perm[...] = order_rows[...].astype(F32).T.astype(BF16)

    groups = (slice(0, half), slice(half, pairs))
    joined = 2 if chunks % 2 == 0 else 1
    spans = [lanes(c, joined) for c in range(0, chunks, joined)]
    seen = set()

    def have(g, j):
        for at in range(g * mid, (g + 1) * mid):
            for c in range(j * joined, (j + 1) * joined):
                key = (0, 0) if at == 0 else (c, at)
                if key not in seen:
                    seen.add(key)
                    if at == 0:
                        own_pair(peer).wait_recv()
                    else:
                        pair_copy(c, at, peer).wait_recv()

    def have_w():
        if "w" not in seen:
            seen.add("w")
            for h in range(2):
                w_copy(h).wait()

    tile = rows // 2 if rows % 32 == 0 else rows
    tiles = [slice(r, r + tile) for r in range(0, rows, tile)]

    def term(g, j, h, at):
        return lax.dot_general(
            w_buf[h, at, spans[j]], x_buf[h, groups[g], spans[j]], NT, preferred_element_type=F32
        )

    def turned(g):
        for at in tiles:
            both = jnp.dot(
                t_buf[g, at, :], order_rows[groups[g], :], preferred_element_type=F32
            ).astype(BF16)
            for h in range(2):
                part = both[:, h * half:(h + 1) * half]
                if g == 0:
                    pa_buf[h, at, :] = part
                else:
                    p_buf[h, at, :] = part + pa_buf[h, at, :]

    def early(j):
        def run():
            have_w()
            have(0, j)
            for at in tiles:
                total = term(0, j, 0, at) + term(0, j, 1, at)
                if j > 0:
                    total = total + acc[0, at, :]
                if j < len(spans) - 1:
                    acc[0, at, :] = total
                else:
                    t_buf[0, at, :] = total.astype(BF16)
            if j == len(spans) - 1:
                turned(0)
        return run

    def late(j):
        def run():
            have_w()
            if j > 0:
                have(1, j - 1)
            for at in tiles:
                parts = []
                if j > 0:
                    parts = [acc[1, at, :], term(1, j - 1, peer, at)]
                if j < len(spans):
                    acc[1, at, :] = sum(parts + [term(1, j, core, at)])
                else:
                    t_buf[1, at, :] = sum(parts).astype(BF16)
            if j == len(spans):
                turned(1)
        return run

    def order_own(g, j):
        def run():
            part = jnp.dot(
                perm[:, groups[g]], x_buf[core, groups[g], spans[j]], preferred_element_type=F32
            )
            if g == 1:
                part = part + e_buf[:, spans[j]].astype(F32)
            e_buf[:, spans[j]] = part.astype(BF16)
        return run

    def arrival(j, d):
        return max(
            (d - 1) * chunks + sequence[side].index(c)
            for c in range(j * joined, (j + 1) * joined) for side in range(2)
            if d < mid or c % 2 == side
        )

    turn = (mid + 1) // 2
    todo = []
    for j in range(len(spans)):
        todo.append((arrival(j, turn) + 1 + j, early(j)))
        todo.append((arrival(j, turn) + 2 + j, order_own(0, j)))
    for j in range(len(spans)):
        todo.append((arrival(j, mid), late(j)))
        todo.append((arrival(j, mid), order_own(1, j)))
    todo.append((mid * chunks, late(len(spans))))

    slot = 0
    for d in range(1, mid + 1):
        for i in range(chunks):
            moved = False
            for side in range(2):
                c = sequence[side][i]
                if d <= reach(c, side):
                    moved = True
                    ring_copy(c, d - 1, side).wait_recv()
                    if d < reach(c, side):
                        ring_copy(c, d, side).start()
                    pair_copy(c, spot(d, side), core).start()
            if moved and todo and todo[0][0] <= slot:
                todo.pop(0)[1]()
                if d == mid and todo and todo[0][0] <= slot - i:
                    todo.pop(0)[1]()
            slot += 1
    for _, run in todo:
        run()

    size = k_send.shape[1]
    count = size // per
    near = me // mid
    local = me % mid
    parts = half // size
    pieces = []
    for b in range(2):
        for s in range(parts):
            pieces.append((b, s))

    def piece_rows(b, s):
        return pl.ds(pl.multiple_of(b * half + s * size, size), size)

    def half_copy(i):
        return pltpu.make_async_remote_copy(
            src_ref=k_send.at[i], dst_ref=k_peer.at[i], send_sem=half_send.at[i],
            recv_sem=half_recv.at[i], device_id={"gvec": peer}, device_id_type=MESH,
        )

    def out_copy(target, slot):
        return pltpu.make_async_remote_copy(
            src_ref=k_red.at[pl.ds(pl.multiple_of(target * per, per), per), :],
            dst_ref=rows_in.at[me], send_sem=out_send.at[slot], recv_sem=out_recv.at[me],
            device_id={"freq": target}, device_id_type=MESH,
        )

    far = half // size
    def emit(i):
        k_send[i] = jnp.dot(e_buf[piece_rows(*pieces[i]), :], p_buf[peer], preferred_element_type=F32)
        half_copy(i).start()

    def keep(i):
        k_own[i] = jnp.dot(e_buf[piece_rows(*pieces[i]), :], p_buf[core], preferred_element_type=F32)

    targets = []

    def finish(i):
        b, s = pieces[i]
        half_copy(i).wait_recv()
        k_red[piece_rows(b, s), :] = (k_own[i] + k_peer[i]).astype(BF16)
        for t in range(count):
            target = b * mid + s * count + t
            slot = len(targets)

            @pl.when(target != me)
            def _():
                out_copy(target, slot).start()

            targets.append(target)

    last = len(pieces)
    for i in range(last + 1):
        if i < last:
            emit(i)
            keep(i)
        if i >= 1:
            finish(i - 1)
    rows_in[me] = k_red[mine, :]

    for c in range(chunks):
        for side in range(2):
            for d in range(reach(c, side)):
                ring_copy(c, d, side).wait_send()
        for at in range(1, n):
            pair_copy(c, at, core).wait_send()
    own_pair(core).wait_send()
    for i in range(len(pieces)):
        half_copy(i).wait_send()

    def arrived(t):
        source = near * mid + (local + t) % mid if t < mid else (1 - near) * mid + (local + t) % mid
        pltpu.make_async_remote_copy(
            src_ref=rows_in.at[source], dst_ref=rows_in.at[source],
            send_sem=out_send.at[0], recv_sem=out_recv.at[source],
            device_id={"freq": source}, device_id_type=MESH,
        ).wait_recv()
        return source

    def weighted(o, sources):
        return sum(quad_table[quad_index[o, f]] * rows_in[f].astype(F32) for f in sources)

    sources = [me]
    for t in range(1, mid):
        sources.append(arrived(t))
    for o in range(out.shape[0]):
        out[o] = weighted(o, sources)
    for t in range(mid, n, 2):
        sources = [arrived(t), arrived(t + 1)]
        for o in range(out.shape[0]):
            out[o] = out[o] + weighted(o, sources)

    for slot, target in enumerate(targets):
        @pl.when(target != me)
        def _():
            out_copy(target, slot).wait_send()


def body(n, screened, densities, pair_order, quad_index, quad_table):
    rows, per = densities.shape
    pairs = n * per
    half = pairs // 2
    mid = n // 2
    chunks = next(c for c in (4, 3, 2, 1) if rows % (c * 128) == 0 or c == 1)
    width = rows // chunks
    size = half // 2 if mid % 2 == 0 and (half // 2) % 16 == 0 else half
    count = half // size * 2
    energies = quad_index.shape[0]
    dma = pltpu.SemaphoreType.DMA
    hbm = pl.BlockSpec(memory_space=pl.ANY)
    vmem = pl.BlockSpec(memory_space=pltpu.VMEM)
    smem = pl.BlockSpec(memory_space=pltpu.SMEM)
    return pl.pallas_call(
        functools.partial(kernel, n, chunks),
        out_shape=pltpu.VMEM((energies, per, half), F32),
        in_specs=[hbm, hbm, vmem, smem, smem],
        out_specs=vmem,
        scratch_shapes=[
            pltpu.VMEM((2, rows, rows), BF16),
            pltpu.VMEM((2, pairs, rows), BF16),
            pltpu.VMEM((pairs, rows), BF16),
            pltpu.VMEM((2, rows, half), F32),
            pltpu.VMEM((2, rows, half), BF16),
            pltpu.VMEM((2, rows, half), BF16),
            pltpu.VMEM((2, rows, half), BF16),
            pltpu.VMEM((pairs, pairs), BF16),
            pltpu.VMEM((pairs, pairs), BF16),
            pltpu.VMEM((count, size, half), F32),
            pltpu.VMEM((count, size, half), F32),
            pltpu.VMEM((count, size, half), F32),
            pltpu.VMEM((pairs, half), BF16),
            pltpu.VMEM((n, per, half), BF16),
            dma((1,)), dma((2,)),
            dma((chunks, n)), dma((chunks, n)),
            dma((1,)), dma((1,)),
            dma((chunks, n)), dma((chunks, n)),
            dma((count,)), dma((count,)), dma((n,)), dma((n,)),
        ],
        compiler_params=pltpu.CompilerParams(
            collective_id=0, has_side_effects=True, vmem_limit_bytes=56 * 1024 * 1024
        ),
    )(screened, densities.T, pair_order[None, :], quad_index, quad_table)


def solution(mesh):
    placed = (P(("groups", "freq"), "gvec", None), P(("groups", "gvec"), "freq"), P(), P(), P())
    return jax.shard_map(
        functools.partial(body, mesh.shape["freq"]), mesh=mesh, in_specs=placed,
        out_specs=P("groups", "freq", "gvec"), check_vma=False,
    )
```
